32 devices in a mesh: dp: 8 (over z, y), tr: 2 (over core), tc: 2 (over x).
Axes of the slice: x: 2, y: 2, z: 4, core: 2. Of those that a mesh axis runs over, the one named last changes fastest.
Arguments:
- activations: bfloat16 [4096, 4096], P('dp', ('tr', 'tc')), may hold values from -16.8 to 16.8, as said below
- gradients: bfloat16 [4096, 7168], P('dp', ('tr', 'tc')), may hold values from -16.8 to 16.8, as said below
- old_inputs: float32 [4096, 4096], P(('dp', 'tr', 'tc')), may hold values from -3 to 3
- old_gradients: float32 [7168, 7168], P(('dp', 'tr', 'tc')), may hold values from -3 to 3
Outputs:
- input_factor: float32 [4096, 4096], P(('dp', 'tr', 'tc'))
- grad_factor: float32 [7168, 7168], P(('dp', 'tr', 'tc'))
The draws below stay inside these ranges and needn't reach their ends.
Inputs may be any that keep to these rules, and one draw needn't show every extreme that they name: `activations`: real-valued samples. `gradients`: real-valued samples.
All inputs are finite; a program needn't handle non-finite values.
Results may differ from the reference program's by a relative error of at most 0.0045.
Values may be sent and summed in bfloat16 or wider, within the bound.
A program may use at most 192 MiB of HBM per device.

```python
import jax
import jax.numpy as jnp
from jax import lax

D = 4096
FF = 7168
TOK_DEV = 512
N_DP = 8


def spiked(key, width):
    first = jax.random.fold_in(key, 0)
    third = jax.random.fold_in(key, 2)
    rows_total = TOK_DEV * N_DP
    base = jnp.clip(jax.random.normal(first, (rows_total, width), jnp.float32), -6.0, 6.0)
    pairing = jax.random.permutation(third, N_DP).astype(jnp.int32)
    replica = jnp.arange(rows_total, dtype=jnp.int32) // TOK_DEV
    block = jnp.arange(width, dtype=jnp.int32) // (width // N_DP)
    target = jnp.take(pairing, replica)
    boost = jnp.where(target[:, None] == block[None, :], 2.0, 1.0)
    return (base * boost).astype(jnp.bfloat16)


def draw_activations(key, part):
    return spiked(jax.random.fold_in(key, 11), D)


def draw_gradients(key, part):
    return spiked(jax.random.fold_in(key, 23), FF)


def levels(key, dims, cuts, low, largest):
    factor_of, own = 1.0, jax.random.fold_in(key, 6)
    for axis_at, blocks in cuts:
        heights = jnp.exp(jax.random.uniform(jax.random.fold_in(own, axis_at), (blocks,), jnp.float32, low / len(cuts), largest / len(cuts)))
        factor_of = factor_of * jnp.repeat(heights, dims[axis_at] // blocks).reshape([-1 if axis == axis_at else 1 for axis in range(len(dims))])
    return factor_of


def bell_draw(own_key, shape, scale, most, cuts=(), kind=jnp.bfloat16):
    entries = scale * jax.random.normal(own_key, shape, jnp.float32)
    if cuts:
        entries = entries * levels(own_key, shape, cuts, -0.22, 0.18)
    return jnp.clip(entries, -most, most).astype(kind)


def setup_inputs(seed: int = 0) -> dict:
    key_list = jax.random.split(jax.random.key(seed), 5)
    activations = draw_activations(jax.random.fold_in(key_list[4], 71), 0)
    gradients = draw_gradients(jax.random.fold_in(key_list[4], 71), 0)
    old_inputs = bell_draw(key_list[2], (D, D), 0.5, 3.0, ((0, 32),), jnp.float32)
    old_gradients = bell_draw(key_list[3], (FF, FF), 0.5, 3.0, ((0, 32),), jnp.float32)
    return {"activations": activations, "gradients": gradients, "old_inputs": old_inputs, "old_gradients": old_gradients}


def replica_sum(samples, tokens_all):
    columns = samples.shape[1]
    replicas = samples.reshape(N_DP, TOK_DEV, columns)

    def accumulate(running, replica_rows):
        partial_value = (jnp.dot(replica_rows.T, replica_rows, preferred_element_type=jnp.float32) / tokens_all).astype(jnp.bfloat16)
        return running + partial_value.astype(jnp.float32), None

    running, _ = lax.scan(accumulate, jnp.zeros((columns, columns), jnp.float32), replicas)
    return running


def reference(activations, gradients, old_inputs, old_gradients):
    tokens_all = N_DP * TOK_DEV
    input_new = replica_sum(activations, tokens_all)
    gradient_new = replica_sum(gradients, tokens_all)
    return (0.5 * old_inputs + 0.5 * input_new, 0.5 * old_gradients + 0.5 * gradient_new)
```

```python
import functools

import jax
import jax.numpy as jnp
from jax import lax
from jax.experimental import pallas as pl
from jax.experimental.pallas import tpu as pltpu
from jax.sharding import Mesh, PartitionSpec as P

GROUP = (2, 2, 2)
REPLICA = ("q", "zh", "zl", "y")
AXES = REPLICA + ("tr", "tc")
F32, BF16 = jnp.float32, jnp.bfloat16
LANES, STEP = 128, 256
CHUNKS = (4, 2)


def split_mesh(mesh):
    size = mesh.shape["dp"] // 8
    rest = tuple(mesh.shape[name] for name in mesh.axis_names[1:])
    return Mesh(mesh.devices.reshape((size,) + GROUP + rest), AXES)


class Place:
    def __init__(self):
        for name in AXES:
            setattr(self, name, lax.axis_index(name))
        self.replica = self.zh * 4 + self.zl * 2 + self.y
        self.partner = self.zh * 4 + (1 - self.zl) * 2 + self.y

    def flip(self, *names):
        return {name: 1 - getattr(self, name) for name in names}


class Factor:
    def __init__(self, at, chunks, groups, samples, out, refs):
        self.at, self.chunks, self.groups = at, chunks, groups
        self.samples, self.out = samples, out
        (self.wide, self.left, self.left_in, self.pair, self.side, self.pair_in, self.side_in,
         self.total, self.local_sem, self.send_sem, self.recv_sem) = refs
        self.tokens, self.width = samples.shape
        self.rows = self.side.shape[0]
        self.half = 2 * self.width
        self.used, self.sent = {}, []

    def sem(self, *key):
        return self.used.setdefault(key, len(self.used))

    def spot(self, t, y, c, k):
        size = self.tokens // self.chunks
        row = pl.multiple_of((2 * t + y) * self.tokens + k * size, size)
        return self.wide.at[pl.ds(row, size), pl.ds(pl.multiple_of(c * self.width, LANES), self.width)]

    def own(self, k):
        size = self.tokens // self.chunks
        return self.samples.at[pl.ds(k * size, size)]

    def copy(self, key, source, target, device, recv=None):
        at = self.sem(*key)
        copy = pltpu.make_async_remote_copy(
            src_ref=source,
            dst_ref=target,
            send_sem=self.send_sem.at[at],
            recv_sem=self.recv_sem.at[at if recv is None else recv],
            device_id=device,
            device_id_type=pl.DeviceIdType.MESH,
        )
        return copy

    def start(self, *args):
        copy = self.copy(*args)
        copy.start()
        self.sent.append(copy)
        return copy

    def far(self, k):
        self.start(("far", k), self.own(k), self.spot(1, self.at.y, self.at.tc, k), self.at.flip("zh"))

    def far_wait(self, k):
        here = self.spot(1, self.at.y, self.at.tc, k)
        self.copy(("far", k), here, here, self.at.flip("zh")).wait_recv()

    def direct(self, t, k):
        here = self.spot(t, self.at.y, self.at.tc, k)
        source = here if t else self.own(k)
        for name in ("tc", "y"):
            self.start((name, t, k), source, here, self.at.flip(name))

    def direct_wait(self, t, k, name):
        y = self.at.y if name == "tc" else 1 - self.at.y
        c = 1 - self.at.tc if name == "tc" else self.at.tc
        here = self.spot(t, y, c, k)
        self.copy((name, t, k), here, here, self.at.flip(name)).wait_recv()
        return here

    def relay(self, t, k):
        first, then = (("tc", "y"), ("y", "tc"))[k % 2]
        here = self.direct_wait(t, k, first)
        self.start(("relay", t, k), here, here, self.at.flip(then))

    def rest_wait(self, t, k):
        self.direct_wait(t, k, ("y", "tc")[k % 2])
        here = self.spot(t, 1 - self.at.y, 1 - self.at.tc, k)
        self.copy(("relay", t, k), here, here, self.at.flip("y")).wait_recv()

    def local(self):
        y, c = self.at.y, self.at.tc
        row = pl.multiple_of(y * self.tokens, self.tokens)
        target = self.wide.at[
            pl.ds(row, self.tokens), pl.ds(pl.multiple_of(c * self.width, LANES), self.width)
        ]
        return pltpu.make_async_copy(self.samples, target, self.local_sem.at[0])

    def pick_left(self, groups_rows):
        at, rows = self.at, self.rows
        each = groups_rows
        span = 4 * each
        window = span if span % LANES == 0 else -(-span // LANES) * LANES + LANES
        features = lax.broadcasted_iota(jnp.int32, (rows, window), 1)
        line = lax.broadcasted_iota(jnp.int32, (rows, window), 0)
        for s, replica in ((0, at.replica), (1, at.partner)):
            picks, starts = [], []
            for group in range(self.groups):
                offset = (group * 8 + replica) * span - at.tr * self.half
                start = jnp.clip(offset // LANES * LANES, 0, self.half - window)
                starts.append(pl.multiple_of(start, LANES))
                for core in range(2):
                    wanted = offset + (core * 2 + at.tc) * each - group * each - start
                    hit = features == line + wanted
                    if self.groups > 1:
                        hit &= (line >= group * each) & (line < (group + 1) * each)
                    picks.append(jnp.where(hit, 1.0, 0.0).astype(BF16))

            for core in range(2):
                def block(b, carry, s=s, core=core, picks=picks, starts=starts):
                    tokens = pl.ds(pl.multiple_of(b * self.tokens, self.tokens), self.tokens)
                    total = jnp.zeros((rows, self.tokens), F32)
                    for group in range(self.groups):
                        total += lax.dot_general(
                            picks[2 * group + core],
                            self.wide[tokens, pl.ds(starts[group], window)],
                            (((1,), (1,)), ((), ())),
                            preferred_element_type=F32,
                        )
                    self.left[s, core * rows:(core + 1) * rows, tokens] = total.astype(BF16)
                    return carry

                lax.fori_loop(0, 4, block, 0)

    def make_left(self, groups_rows):
        other = self.at.flip("tr")
        if self.groups == 1:
            mine = self.at.tr == self.at.zh
            copy = self.copy(("left",), self.left, self.left, other)

            @pl.when(mine)
            def _():
                self.pick_left(groups_rows)
                copy.start()

            @pl.when(jnp.logical_not(mine))
            def _():
                copy.wait_recv()

            self.left_copy = (mine, copy)
        else:
            self.pick_left(groups_rows)
            copy = self.copy(("left",), self.left, self.left_in, other)
            copy.start()
            copy.wait()
            self.left[...] = self.left[...] + self.left_in[...]
            self.left_copy = None

    def products(self, scale):
        at, rows, width = self.at, self.rows, self.width
        for part in range(2):
            def pair(i, carry, part=part):
                columns = pl.ds(pl.multiple_of(part * width + i * STEP, STEP), STEP)
                product = jnp.dot(self.left[1], self.wide[:, columns], preferred_element_type=F32)
                self.pair[:, columns] = (product * scale).astype(BF16)
                return carry

            lax.fori_loop(0, width // STEP, pair, 0)
            columns = pl.ds(part * width, width)
            for core in range(2):
                device = dict(at.flip("zl"), tr=core)
                self.start(
                    ("pair", part, core),
                    self.pair.at[pl.ds(core * rows, rows), columns],
                    self.pair_in.at[at.tr, :, columns],
                    device,
                    self.pair_slot(part, at.tr),
                )
        mine = pl.ds(pl.multiple_of(at.tr * rows, 16), rows)
        others = pl.ds(pl.multiple_of((1 - at.tr) * rows, 16), rows)

        def side(i, carry):
            columns = pl.ds(pl.multiple_of(i * STEP, STEP), STEP)
            product = jnp.dot(self.left[0, others, :], self.wide[:, columns], preferred_element_type=F32)
            self.side[:, columns] = (product * scale).astype(BF16)
            return carry

        lax.fori_loop(0, self.half // STEP, side, 0)
        self.start(("side",), self.side, self.side_in, at.flip("tr"))

        def own(i, carry):
            columns = pl.ds(pl.multiple_of(i * STEP, STEP), STEP)
            product = jnp.dot(self.left[0, mine, :], self.wide[:, columns], preferred_element_type=F32)
            place = pl.ds(pl.multiple_of(at.tr * self.half + i * STEP, STEP), STEP)
            self.total[:, place] = product * scale
            return carry

        lax.fori_loop(0, self.half // STEP, own, 0)

    def pair_slot(self, part, core):
        return self.sem("pair", part, 0) + core

    def finish(self):
        at = self.at
        self.copy(("side",), self.side, self.side_in, at.flip("tr")).wait_recv()

        def side(i, carry):
            columns = pl.ds(pl.multiple_of(i * STEP, STEP), STEP)
            place = pl.ds(pl.multiple_of((1 - at.tr) * self.half + i * STEP, STEP), STEP)
            self.total[:, place] = self.side_in[:, columns].astype(F32)
            return carry

        lax.fori_loop(0, self.half // STEP, side, 0)
        outs = []
        for part in range(2):
            for core in range(2):
                here = self.pair_in.at[core, :, pl.ds(part * self.width, self.width)]
                self.copy(("pair", part, core), here, here, dict(at.flip("zl"))).wait_recv()

                def add(i, carry, part=part, core=core):
                    columns = pl.ds(pl.multiple_of(part * self.width + i * STEP, STEP), STEP)
                    place = pl.ds(pl.multiple_of(core * self.half + part * self.width + i * STEP, STEP), STEP)
                    self.total[:, place] += self.pair_in[core, :, columns].astype(F32)
                    return carry

                lax.fori_loop(0, self.width // STEP, add, 0)
                place = pl.ds(core * self.half + part * self.width, self.width)
                copy = pltpu.make_async_copy(
                    self.total.at[:, place], self.out.at[:, place], self.local_sem.at[1 + 2 * part + core]
                )
                copy.start()
                outs.append(copy)
        return outs

    def drain(self):
        for copy in self.sent:
            copy.wait_send()
        if self.left_copy is not None:
            mine, copy = self.left_copy

            @pl.when(mine)
            def _():
                copy.wait_send()


def kernel(groups, each, scale, grads, acts, out_g, out_a, *scratch):
    at = Place()
    barrier = pltpu.get_barrier_semaphore()
    peers = [at.flip(name) for name in ("tc", "y", "zh", "tr")]
    peers += [dict(at.flip("zl"), tr=core) for core in range(2)]
    for peer in peers:
        pl.semaphore_signal(barrier, inc=1, device_id=peer, device_id_type=pl.DeviceIdType.MESH)
    pl.semaphore_wait(barrier, len(peers))

    count = len(scratch) // 2
    g = Factor(at, CHUNKS[0], groups, grads, out_g, scratch[:count])
    a = Factor(at, CHUNKS[1], groups, acts, out_a, scratch[count:])

    for factor in (g, a):
        for k in range(factor.chunks):
            factor.far(k)
    for k in range(g.chunks):
        g.direct(0, k)
    locals_ = [factor.local() for factor in (g, a)]
    for copy in locals_:
        copy.start()

    half = g.chunks // 2
    for k in range(half):
        g.relay(0, k)
    g.far_wait(0)
    g.direct(1, 0)
    for k in range(half, g.chunks):
        g.relay(0, k)
    for k in range(1, g.chunks):
        g.far_wait(k)
        g.direct(1, k)
        if k >= 2:
            g.relay(1, k - 2)
    for k in range(g.chunks - 2, g.chunks):
        g.relay(1, k)
    for k in range(a.chunks):
        a.direct(0, k)
    for copy in locals_:
        copy.wait()
    for t in range(2):
        for k in range(g.chunks):
            g.rest_wait(t, k)
    g.make_left(each[0])
    g.products(scale)
    for k in range(a.chunks):
        a.far_wait(k)
        a.direct(1, k)
    for t in range(2):
        for k in range(a.chunks):
            a.relay(t, k)
    for t in range(2):
        for k in range(a.chunks):
            a.rest_wait(t, k)
    a.make_left(each[1])
    a.products(scale)
    outs = g.finish() + a.finish()
    for factor in (g, a):
        factor.drain()
    for copy in outs:
        copy.wait()


def scratch_of(samples, rows, groups, chunks):
    tokens, width = samples.shape
    half = 2 * width
    left = pltpu.VMEM((2, 2 * rows, 4 * tokens), BF16)
    copies = 7 * chunks + 6
    return [
        pltpu.VMEM((4 * tokens, half), BF16),
        left,
        left if groups > 1 else pltpu.VMEM((16, LANES), BF16),
        pltpu.VMEM((2 * rows, half), BF16),
        pltpu.VMEM((rows, half), BF16),
        pltpu.VMEM((2, rows, half), BF16),
        pltpu.VMEM((rows, half), BF16),
        pltpu.VMEM((rows, 2 * half), F32),
        pltpu.SemaphoreType.DMA((5,)),
        pltpu.SemaphoreType.DMA((copies,)),
        pltpu.SemaphoreType.DMA((copies,)),
    ]


def body(activations, gradients, old_inputs, old_gradients):
    groups = lax.axis_size("q")
    tokens = activations.shape[0] * lax.axis_size(REPLICA)
    samples, olds = (gradients, activations), (old_gradients, old_inputs)
    each = tuple(old.shape[0] for old in olds)
    scratch = []
    for block, rows, chunks in zip(samples, each, CHUNKS):
        scratch += scratch_of(block, groups * rows, groups, chunks)
    new = pl.pallas_call(
        functools.partial(kernel, groups, each, 1.0 / tokens),
        out_shape=tuple(
            jax.ShapeDtypeStruct((groups * old.shape[0], old.shape[1]), F32) for old in olds
        ),
        in_specs=[pl.BlockSpec(memory_space=pltpu.HBM)] * 2,
        out_specs=(pl.BlockSpec(memory_space=pltpu.HBM),) * 2,
        scratch_shapes=scratch,
        compiler_params=pltpu.CompilerParams(
            collective_id=0, has_side_effects=True, vmem_limit_bytes=60 * 2**20
        ),
        name="gram",
    )(*samples)
    outs = []
    for total, old in zip(new, olds):
        if groups > 1:
            total = lax.psum_scatter(total, "q", scatter_dimension=0, tiled=True)
        outs.append(0.5 * old + 0.5 * total)
    return outs[1], outs[0]


def solution(mesh):
    rows = REPLICA + ("tr", "tc")
    return jax.shard_map(
        body,
        mesh=split_mesh(mesh),
        in_specs=(
            P(REPLICA, ("tr", "tc")),
            P(REPLICA, ("tr", "tc")),
            P(rows, None),
            P(rows, None),
        ),
        out_specs=(P(rows, None), P(rows, None)),
        check_vma=False,
    )
```

```python
import functools

import jax
import jax.numpy as jnp
from jax import lax
from jax.experimental import pallas as pl
from jax.experimental.pallas import tpu as pltpu
from jax.sharding import Mesh, PartitionSpec as P

GROUP = (2, 2, 2)
REPLICA = ("q", "zh", "zl", "y")
AXES = REPLICA + ("tr", "tc")
F32, BF16 = jnp.float32, jnp.bfloat16
LANES, STEP, VMEM = 128, 256, 60 * 2**20
CHUNKS = (4, 2)


def split_mesh(mesh):
    size = mesh.shape["dp"] // 8
    rest = tuple(mesh.shape[name] for name in mesh.axis_names[1:])
    return Mesh(mesh.devices.reshape((size,) + GROUP + rest), AXES)


class Place:
    def __init__(self):
        for name in AXES:
            setattr(self, name, lax.axis_index(name))
        self.replica = self.zh * 4 + self.zl * 2 + self.y
        self.partner = self.zh * 4 + (1 - self.zl) * 2 + self.y

    def flip(self, *names):
        return {name: 1 - getattr(self, name) for name in names}


class Factor:
    def __init__(self, at, chunks, groups, each, samples, old, total, refs):
        self.at, self.chunks, self.groups, self.each = at, chunks, groups, each
        self.samples, self.old, self.total = samples, old, total
        (self.wide, self.left, self.left_in, self.pair, self.side, self.pair_in, self.side_in,
         self.block, self.local_sem, self.send_sem, self.recv_sem) = refs
        self.tokens, self.width = samples.shape
        self.rows = self.side.shape[0]
        self.half = 2 * self.width
        self.fold = groups == 1
        keys = [("far", k) for k in range(chunks)]
        keys += [(n, t, k) for n in ("tc", "y", "relay") for t in range(2) for k in range(chunks)]
        keys += [("left", t) for t in range(2)] + [("side",)]
        keys += [("pair", part, core) for part in range(2) for core in range(2)]
        self.keys = {key: i for i, key in enumerate(keys)}
        self.sent, self.far_sent, self.left_sent = [], [], []

    def sem(self, *key):
        return self.keys[key]

    def spot(self, t, y, c, k):
        size = self.tokens // self.chunks
        row = pl.multiple_of((2 * t + y) * self.tokens + k * size, size)
        return self.wide.at[pl.ds(row, size), pl.ds(pl.multiple_of(c * self.width, LANES), self.width)]

    def own(self, k):
        size = self.tokens // self.chunks
        return self.samples.at[pl.ds(k * size, size)]

    def copy(self, key, source, target, device, recv=None):
        at = self.sem(*key)
        copy = pltpu.make_async_remote_copy(
            src_ref=source,
            dst_ref=target,
            send_sem=self.send_sem.at[at],
            recv_sem=self.recv_sem.at[at if recv is None else recv],
            device_id=device,
            device_id_type=pl.DeviceIdType.MESH,
        )
        return copy

    def start(self, *args):
        copy = self.copy(*args)
        copy.start()
        self.sent.append(copy)
        return copy

    def far(self, k):
        here = self.spot(1, self.at.y, self.at.tc, k)
        self.far_sent.append(self.start(("far", k), self.own(k), here, self.at.flip("zh")))

    def far_left(self):
        for copy in self.far_sent:
            copy.wait_send()
        self.sent = [copy for copy in self.sent if not any(copy is one for one in self.far_sent)]

    def far_wait(self, k):
        here = self.spot(1, self.at.y, self.at.tc, k)
        self.copy(("far", k), here, here, self.at.flip("zh")).wait_recv()

    def direct(self, t, k):
        here = self.spot(t, self.at.y, self.at.tc, k)
        source = here if t else self.own(k)
        for name in ("tc", "y"):
            self.start((name, t, k), source, here, self.at.flip(name))

    def direct_wait(self, t, k, name):
        y = self.at.y if name == "tc" else 1 - self.at.y
        c = 1 - self.at.tc if name == "tc" else self.at.tc
        here = self.spot(t, y, c, k)
        self.copy((name, t, k), here, here, self.at.flip(name)).wait_recv()
        return here

    def relay(self, t, k):
        first, then = (("tc", "y"), ("y", "tc"))[k % 2]
        here = self.direct_wait(t, k, first)
        self.start(("relay", t, k), here, here, self.at.flip(then))

    def rest_wait(self, t, k):
        self.direct_wait(t, k, ("y", "tc")[k % 2])
        here = self.spot(t, 1 - self.at.y, 1 - self.at.tc, k)
        self.copy(("relay", t, k), here, here, self.at.flip("y")).wait_recv()

    def local(self):
        y, c = self.at.y, self.at.tc
        row = pl.multiple_of(y * self.tokens, self.tokens)
        target = self.wide.at[
            pl.ds(row, self.tokens), pl.ds(pl.multiple_of(c * self.width, LANES), self.width)
        ]
        copies = [pltpu.make_async_copy(self.samples, target, self.local_sem.at[0])]
        if self.fold:
            copies.append(pltpu.make_async_copy(self.old, self.total, self.local_sem.at[1]))
        return copies

    def pick_left(self, t):
        at, rows, each = self.at, self.rows, self.each
        span = 4 * each
        window = span if span % LANES == 0 else -(-span // LANES) * LANES + LANES
        features = lax.broadcasted_iota(jnp.int32, (rows, window), 1)
        line = lax.broadcasted_iota(jnp.int32, (rows, window), 0)
        for s, replica in ((0, at.replica), (1, at.partner)):
            picks, starts = [], []
            for group in range(self.groups):
                offset = (group * 8 + replica) * span - at.tr * self.half
                start = jnp.clip(offset // LANES * LANES, 0, self.half - window)
                starts.append(pl.multiple_of(start, LANES))
                both = []
                for core in range(2):
                    wanted = offset + (core * 2 + at.tc) * each - group * each - start
                    hit = features == line + wanted
                    if self.groups > 1:
                        hit &= (line >= group * each) & (line < (group + 1) * each)
                    both.append(jnp.where(hit, 1.0, 0.0).astype(BF16))
                picks.append(jnp.concatenate(both, axis=0))

            def block(b, carry, s=s, picks=picks, starts=starts):
                tokens = pl.ds(pl.multiple_of((2 * t + b) * self.tokens, self.tokens), self.tokens)
                total = 0.0
                for pick, start in zip(picks, starts):
                    total += lax.dot_general(
                        pick,
                        self.wide[tokens, pl.ds(start, window)],
                        (((1,), (1,)), ((), ())),
                        preferred_element_type=F32,
                    )
                self.left[s, :, tokens] = total.astype(BF16)
                return carry

            lax.fori_loop(0, 2, block, 0)

    def left_copy(self, t):
        tokens = pl.ds(2 * t * self.tokens, 2 * self.tokens)
        target = self.left if self.groups == 1 else self.left_in
        return ("left", t), self.left.at[:, :, tokens], target.at[:, :, tokens], self.at.flip("tr")

    def make_left(self, t, mine):
        if mine or self.groups > 1:
            self.pick_left(t)
            self.left_sent.append(self.start(*self.left_copy(t)))

    def get_left(self, mine):
        if not mine or self.groups > 1:
            for t in range(2):
                self.copy(*self.left_copy(t)).wait_recv()
        if self.groups > 1:
            for copy in self.left_sent:
                copy.wait_send()
            self.sent = [copy for copy in self.sent if not any(copy is one for one in self.left_sent)]
            self.left[...] = self.left[...] + self.left_in[...]

    def product(self, s, columns):
        return jnp.dot(self.left[s], self.wide[:, columns], preferred_element_type=F32)

    def pair_products(self, scale):
        at, rows, width = self.at, self.rows, self.width
        for part in range(2):
            def pair(i, carry, part=part):
                columns = pl.ds(pl.multiple_of(part * width + i * STEP, STEP), STEP)
                self.pair[:, columns] = (self.product(1, columns) * scale).astype(BF16)
                return carry

            lax.fori_loop(0, width // STEP, pair, 0)
            columns = pl.ds(part * width, width)
            for core in range(2):
                self.start(
                    ("pair", part, core),
                    self.pair.at[pl.ds(core * rows, rows), columns],
                    self.pair_in.at[at.tr, :, columns],
                    dict(at.flip("zl"), tr=core),
                    self.sem("pair", part, 0) + at.tr,
                )

    def add(self, place, value, first):
        if self.fold:
            base = 0.5 * self.total[:, place] if first else self.total[:, place]
            self.total[:, place] = base + 0.5 * value
        elif first:
            self.total[:, place] = value
        else:
            self.total[:, place] += value

    def own_products(self, scale):
        at, rows = self.at, self.rows
        mine = pl.ds(pl.multiple_of(at.tr * rows, 16), rows)
        others = pl.ds(pl.multiple_of((1 - at.tr) * rows, 16), rows)

        def own(i, carry):
            columns = pl.ds(pl.multiple_of(i * STEP, STEP), STEP)
            place = pl.ds(pl.multiple_of(at.tr * self.half + i * STEP, STEP), STEP)
            self.block[...] = self.product(0, columns) * scale
            self.side[:, columns] = self.block[others, :].astype(BF16)
            self.add(place, self.block[mine, :], True)
            return carry

        lax.fori_loop(0, self.half // STEP, own, 0)
        self.start(("side",), self.side, self.side_in, at.flip("tr"))

    def finish(self):
        at = self.at
        self.copy(("side",), self.side, self.side_in, at.flip("tr")).wait_recv()

        def side(i, carry):
            columns = pl.ds(pl.multiple_of(i * STEP, STEP), STEP)
            place = pl.ds(pl.multiple_of((1 - at.tr) * self.half + i * STEP, STEP), STEP)
            self.add(place, self.side_in[:, columns].astype(F32), True)
            return carry

        lax.fori_loop(0, self.half // STEP, side, 0)
        for core in range(2):
            for part in range(2):
                here = self.pair_in.at[core, :, pl.ds(part * self.width, self.width)]
                self.copy(("pair", part, core), here, here, at.flip("zl")).wait_recv()

                def add(i, carry, part=part, core=core):
                    columns = pl.ds(pl.multiple_of(part * self.width + i * STEP, STEP), STEP)
                    place = pl.ds(pl.multiple_of(core * self.half + part * self.width + i * STEP, STEP), STEP)
                    self.add(place, self.pair_in[core, :, columns].astype(F32), False)
                    return carry

                lax.fori_loop(0, self.width // STEP, add, 0)

    def drain(self):
        for copy in self.sent:
            copy.wait_send()


def program(lead, at, g, a, scale, flags):
    def tell(i):
        pl.semaphore_signal(flags.at[i], inc=1, device_id=at.flip("tr"), device_id_type=pl.DeviceIdType.MESH)

    def hear(i):
        pl.semaphore_wait(flags.at[i], 1)

    def each(factor, call, *args):
        for k in range(factor.chunks):
            call(*args, k)

    if not lead:
        each(g, g.far)
    each(g, g.direct, 0)
    local = [copy for factor in (g, a) for copy in factor.local()]
    for copy in local:
        copy.start()
    each(g, g.relay, 0)
    for copy in local:
        copy.wait()
    if lead:
        for k in range(g.chunks):
            g.far_wait(k)
            g.direct(1, k)
        hear(0)
        each(g, g.far)
        each(g, g.rest_wait, 0)
        g.make_left(0, lead)
        each(g, g.relay, 1)
        each(g, g.rest_wait, 1)
        tell(1)
        g.make_left(1, lead)
        g.get_left(lead)
        g.pair_products(scale)
        g.own_products(scale)
        each(a, a.direct, 0)
        hear(2)
        each(a, a.far)
        each(a, a.relay, 0)
        for k in range(a.chunks):
            a.far_wait(k)
            a.direct(1, k)
        each(a, a.rest_wait, 0)
        a.make_left(0, lead)
        each(a, a.relay, 1)
        each(a, a.rest_wait, 1)
        tell(3)
        a.make_left(1, lead)
        a.get_left(lead)
        a.pair_products(scale)
        a.own_products(scale)
    else:
        g.far_left()
        tell(0)
        each(g, g.rest_wait, 0)
        g.make_left(0, lead)
        each(g, g.far_wait)
        each(a, a.far)
        hear(1)
        each(g, g.direct, 1)
        each(g, g.relay, 1)
        each(a, a.direct, 0)
        a.far_left()
        tell(2)
        each(g, g.rest_wait, 1)
        g.make_left(1, lead)
        g.get_left(lead)
        g.pair_products(scale)
        each(a, a.relay, 0)
        g.own_products(scale)
        each(a, a.far_wait)
        each(a, a.rest_wait, 0)
        a.make_left(0, lead)
        hear(3)
        each(a, a.direct, 1)
        each(a, a.relay, 1)
        each(a, a.rest_wait, 1)
        a.make_left(1, lead)
        a.get_left(lead)
        a.pair_products(scale)
        a.own_products(scale)
    g.finish()
    a.finish()
    g.drain()
    a.drain()


def kernel(groups, each, scale, *refs):
    at = Place()
    barrier = pltpu.get_barrier_semaphore()
    peers = [at.flip(name) for name in ("tc", "y", "zh", "tr")]
    peers += [dict(at.flip("zl"), tr=core) for core in range(2)]
    for peer in peers:
        pl.semaphore_signal(barrier, inc=1, device_id=peer, device_id_type=pl.DeviceIdType.MESH)
    pl.semaphore_wait(barrier, len(peers))

    samples, refs = refs[:2], refs[2:]
    olds = (None, None)
    if groups == 1:
        olds, refs = refs[:2], refs[2:]
    totals, scratch, flags = refs[:2], refs[2:-1], refs[-1]
    count = len(scratch) // 2

    def run(lead):
        factors = [
            Factor(at, CHUNKS[i], groups, each[i], samples[i], olds[i], totals[i],
                   scratch[i * count:(i + 1) * count])
            for i in range(2)
        ]
        program(lead, at, *factors, scale, flags)

    lead = at.tr == at.zh
    pl.when(lead)(functools.partial(run, True))
    pl.when(jnp.logical_not(lead))(functools.partial(run, False))


def scratch_of(samples, rows, groups, chunks):
    tokens, width = samples.shape
    half = 2 * width
    left = pltpu.VMEM((2, 2 * rows, 4 * tokens), BF16)
    copies = 7 * chunks + 7
    return [
        pltpu.VMEM((4 * tokens, half), BF16),
        left,
        left if groups > 1 else pltpu.VMEM((16, LANES), BF16),
        pltpu.VMEM((2 * rows, half), BF16),
        pltpu.VMEM((rows, half), BF16),
        pltpu.VMEM((2, rows, half), BF16),
        pltpu.VMEM((rows, half), BF16),
        pltpu.VMEM((2 * rows, STEP), F32),
        pltpu.SemaphoreType.DMA((2,)),
        pltpu.SemaphoreType.DMA((copies,)),
        pltpu.SemaphoreType.DMA((copies,)),
    ]


def body(activations, gradients, old_inputs, old_gradients):
    groups = lax.axis_size("q")
    tokens = activations.shape[0] * lax.axis_size(REPLICA)
    samples, olds = (gradients, activations), (old_gradients, old_inputs)
    each = tuple(old.shape[0] for old in olds)
    scratch = []
    for block, rows, chunks in zip(samples, each, CHUNKS):
        scratch += scratch_of(block, groups * rows, groups, chunks)
    scratch.append(pltpu.SemaphoreType.REGULAR((4,)))
    operands = samples + olds if groups == 1 else samples
    new = pl.pallas_call(
        functools.partial(kernel, groups, each, 1.0 / tokens),
        out_shape=tuple(
            jax.ShapeDtypeStruct((groups * old.shape[0], old.shape[1]), F32) for old in olds
        ),
        in_specs=[pl.BlockSpec(memory_space=pltpu.HBM)] * len(operands),
        out_specs=(pl.BlockSpec(memory_space=pltpu.VMEM),) * 2,
        scratch_shapes=scratch,
        compiler_params=pltpu.CompilerParams(
            collective_id=0, has_side_effects=True, vmem_limit_bytes=VMEM
        ),
        name="gram",
    )(*operands)
    if groups > 1:
        new = [lax.psum_scatter(total, "q", scatter_dimension=0, tiled=True) for total in new]
        new = [0.5 * old + 0.5 * total for total, old in zip(new, olds)]
    return new[1], new[0]


def solution(mesh):
    rows = REPLICA + ("tr", "tc")
    return jax.shard_map(
        body,
        mesh=split_mesh(mesh),
        in_specs=(
            P(REPLICA, ("tr", "tc")),
            P(REPLICA, ("tr", "tc")),
            P(rows, None),
            P(rows, None),
        ),
        out_specs=(P(rows, None), P(rows, None)),
        check_vma=False,
    )
```

```python
import functools

import jax
import jax.numpy as jnp
from jax import lax
from jax.experimental import pallas as pl
from jax.experimental.pallas import tpu as pltpu
from jax.sharding import Mesh, PartitionSpec as P

GROUP = (2, 2, 2)
REPLICA = ("q", "zh", "zl", "y")
AXES = REPLICA + ("tr", "tc")
F32, BF16 = jnp.float32, jnp.bfloat16
LANES, STEP = 128, 256
VMEM, WIDE_VMEM = 54 * 2**20, 55 * 2**20
CHUNKS = (4, 2)


def split_mesh(mesh):
    size = mesh.shape["dp"] // 8
    rest = tuple(mesh.shape[name] for name in mesh.axis_names[1:])
    return Mesh(mesh.devices.reshape((size,) + GROUP + rest), AXES)


class Place:
    def __init__(self):
        for name in AXES:
            setattr(self, name, lax.axis_index(name))
        self.replica = self.zh * 4 + self.zl * 2 + self.y
        self.partner = self.zh * 4 + (1 - self.zl) * 2 + self.y

        self.cell = self.tr * 2 + self.tc

    def flip(self, *names):
        return {name: 1 - getattr(self, name) for name in names}


class Factor:
    def __init__(self, at, chunks, groups, each, samples, old, total, refs):
        self.at, self.chunks, self.groups, self.each = at, chunks, groups, each
        self.samples, self.old, self.total = samples, old, total
        (self.wide, self.left, self.left_in, self.pair, self.pair_in, self.sum, self.done,
         self.done_in, self.local_sem, self.send_sem, self.recv_sem, self.ready) = refs
        self.tokens, self.width = samples.shape
        self.lines = self.pair.shape[0]
        self.rows = self.lines // 4
        self.fold = groups == 1
        self.turn = lax.rem(at.tc + at.zl, 2)
        steps = self.width // STEP
        self.parts = ((0, (steps + 1) // 2), ((steps + 1) // 2, steps))
        keys = [("far", k) for k in range(chunks)]
        keys += [("y", t, k) for t in range(2) for k in range(chunks)]
        keys += [(n, t, o) for n in ("cross", "give", "pass") for t in range(2) for o in range(2)]
        keys += [("pair", p) for p in range(2)]
        keys += [("done", p, f) for p in range(2) for f in range(3)]
        keys += [("mix", s, i) for s in range(2) for i in range(2)]
        self.keys = {key: i for i, key in enumerate(keys)}
        self.sent = {}

    def copy(self, key, source, target, device):
        at = self.keys[key]
        return pltpu.make_async_remote_copy(
            src_ref=source,
            dst_ref=target,
            send_sem=self.send_sem.at[at],
            recv_sem=self.recv_sem.at[at],
            device_id=device,
            device_id_type=pl.DeviceIdType.MESH,
        )

    def start(self, key, source, target, device):
        self.sent[key] = self.copy(key, source, target, device)
        self.sent[key].start()

    def leave(self, *key):
        self.sent.pop(key).wait_send()

    def receive(self, key, here):
        self.copy(key, here, here, self.at.flip("tr")).wait_recv()

    def spot(self, t, y, k):
        size = self.tokens // self.chunks
        return self.wide.at[pl.ds(pl.multiple_of((2 * t + y) * self.tokens + k * size, size), size)]

    def own(self, k):
        size = self.tokens // self.chunks
        return self.samples.at[pl.ds(k * size, size)]

    def local(self):
        row = pl.multiple_of(self.at.y * self.tokens, self.tokens)
        target = self.wide.at[pl.ds(row, self.tokens)]
        copies = [pltpu.make_async_copy(self.samples, target, self.local_sem.at[0])]
        if self.fold:
            copies.append(pltpu.make_async_copy(self.old, self.total, self.local_sem.at[1]))
        return copies

    def far(self):
        for k in range(self.chunks):
            self.start(("far", k), self.own(k), self.spot(1, self.at.y, k), self.at.flip("zh"))

    def far_left(self):
        for k in range(self.chunks):
            self.leave("far", k)

    def beside(self, t, k):
        here = self.spot(t, self.at.y, k)
        self.start(("y", t, k), here if t else self.own(k), here, self.at.flip("y"))

    def beside_own(self):
        for k in range(self.chunks):
            self.beside(0, k)

    def beside_left(self):
        for t in range(2):
            for k in range(self.chunks):
                self.leave("y", t, k)

    def beside_far(self):
        for k in range(self.chunks):
            self.receive(("far", k), self.spot(1, self.at.y, k))
            self.beside(1, k)

    def beside_wait(self, t):
        for k in range(self.chunks):
            self.receive(("y", t, k), self.spot(t, 1 - self.at.y, k))

    def stretch(self, t, o):
        y = 1 - self.at.y if o else self.at.y
        return pl.ds(pl.multiple_of((2 * t + y) * self.tokens, self.tokens), self.tokens)

    def pick(self, s, replica, tokens):
        at, rows, each = self.at, self.rows, self.each
        span = 4 * each
        window = span if span % LANES == 0 else -(-span // LANES) * LANES + LANES
        line = lax.broadcasted_iota(jnp.int32, (rows, window), 0)
        feature = lax.broadcasted_iota(jnp.int32, (rows, window), 1)
        total = 0.0
        for group in range(self.groups):
            offset = (group * 8 + replica) * span - at.cell * self.width
            start = pl.multiple_of(jnp.clip(offset // LANES * LANES, 0, self.width - window), LANES)
            cells = []
            for cell in range(4):
                hit = feature == line + (offset - start + (cell - group) * each)
                if self.groups > 1:
                    hit &= (line >= group * each) & (line < (group + 1) * each)
                cells.append(jnp.where(hit, 1.0, 0.0).astype(BF16))
            total += lax.dot_general(
                jnp.concatenate(cells, axis=0),
                self.wide[tokens, pl.ds(start, window)],
                (((1,), (1,)), ((), ())),
                preferred_element_type=F32,
            )
        self.left[s, :, tokens] = total.astype(BF16)

    def give(self, t, o):
        if self.groups > 1:
            return
        at, tokens = self.at, self.stretch(t, o)
        self.pick(self.turn, jnp.where(self.turn == 0, at.replica, at.partner), tokens)
        here = self.left.at[self.turn, :, tokens]
        self.start(("cross", t, o), here, here, at.flip("tc"))
        self.start(("give", t, o), here, here, at.flip("tr"))

    def hand_on(self, t, o):
        if self.groups > 1:
            return
        here = self.left.at[1 - self.turn, :, self.stretch(t, o)]
        self.receive(("cross", t, o), here)
        self.start(("pass", t, o), here, here, self.at.flip("tr"))

    def get_left(self, lead):
        at = self.at
        if self.groups == 1:
            if not lead:
                for t in range(2):
                    for o in range(2):
                        self.receive(("give", t, o), self.left.at[self.turn, :, self.stretch(t, o)])
                        self.receive(("pass", t, o), self.left.at[1 - self.turn, :, self.stretch(t, o)])
            return
        for s, replica in ((0, at.replica), (1, at.partner)):
            def block(b, carry, s=s, replica=replica):
                tokens = pl.ds(pl.multiple_of(b * self.tokens, self.tokens), self.tokens)
                self.pick(s, replica, tokens)
                return carry

            lax.fori_loop(0, 4, block, 0)
        for s in range(2):
            for i, name in enumerate(("tr", "tc")):
                other = at.flip(name)
                pl.semaphore_signal(self.ready.at[i], inc=1, device_id=other, device_id_type=pl.DeviceIdType.MESH)
                pl.semaphore_wait(self.ready.at[i], 1)
                self.start(("mix", s, i), self.left.at[s], self.left_in, other)
                self.receive(("mix", s, i), self.left_in)
                self.leave("mix", s, i)
                self.left[s] = self.left[s] + self.left_in[...]

    def columns(self, part):
        low, high = self.parts[part]
        return pl.ds(low * STEP, (high - low) * STEP)

    def steps(self, part, one):
        low, high = self.parts[part]

        def step(i, carry):
            one(pl.ds(pl.multiple_of(i * STEP, STEP), STEP), i)
            return carry

        lax.fori_loop(low, high, step, 0)

    def product(self, s, columns):
        return jnp.dot(self.left[s], self.wide[:, columns], preferred_element_type=F32)

    def pair_products(self, scale):
        def one(columns, i):
            self.pair[:, columns] = (self.product(1, columns) * scale).astype(BF16)

        for part in range(2):
            self.steps(part, one)
            here = self.columns(part)
            self.start(("pair", part), self.pair.at[:, here], self.pair_in.at[:, here], self.at.flip("zl"))

    def own_products(self, scale):
        def one(columns, i):
            self.sum[:, columns] = self.product(0, columns) * scale

        for part in range(2):
            self.steps(part, one)

    def others(self):
        at = self.at
        for f, (up, over) in enumerate(((0, 1), (1, 0), (1, 1))):
            tr = 1 - at.tr if up else at.tr
            tc = 1 - at.tc if over else at.tc
            yield f, {"tr": tr, "tc": tc}, tr * 2 + tc

    def lot(self, cell):
        return pl.ds(pl.multiple_of(cell * self.rows, 16), self.rows)

    def put(self, cell, i, value):
        place = pl.ds(pl.multiple_of(cell * self.width + i * STEP, LANES), STEP)
        self.total[:, place] = 0.5 * self.total[:, place] + 0.5 * value if self.fold else value

    def spread(self):
        at = self.at

        def one(columns, i):
            value = self.sum[:, columns] + self.pair_in[:, columns].astype(F32)
            self.sum[:, columns] = value
            self.done[:, columns] = value.astype(BF16)
            self.put(at.cell, i, self.sum[self.lot(at.cell), columns])

        for part in range(2):
            here = self.columns(part)
            self.receive(("pair", part), self.pair_in.at[:, here])
            self.steps(part, one)
            for f, device, cell in self.others():
                self.start(
                    ("done", part, f),
                    self.done.at[self.lot(cell), here],
                    self.done_in.at[self.lot(at.cell), here],
                    device,
                )

    def finish(self):
        for part in range(2):
            for f, device, cell in self.others():
                def one(columns, i, cell=cell):
                    self.put(cell, i, self.done_in[self.lot(cell), columns].astype(F32))

                self.receive(("done", part, f), self.done_in.at[self.lot(cell), self.columns(part)])
                self.steps(part, one)

    def drain(self):
        for key in list(self.sent):
            self.leave(*key)


def program(lead, at, g, a, scale, flags):
    def tell(i):
        pl.semaphore_signal(flags.at[i], inc=1, device_id=at.flip("tr"), device_id_type=pl.DeviceIdType.MESH)

    def hear(i):
        pl.semaphore_wait(flags.at[i], 1)

    local = g.local() + a.local()
    if not lead:
        g.far()
    for copy in local:
        copy.start()
    if lead:
        g.beside_own()
        local.pop(0).wait()
        g.give(0, 0)
        g.beside_wait(0)
        g.give(0, 1)
        g.beside_far()
        g.give(1, 0)
        hear(1)
        g.far()
        g.beside_left()
        tell(0)
        g.hand_on(0, 0)
        g.hand_on(0, 1)
        g.beside_wait(1)
        g.give(1, 1)
        for copy in local:
            copy.wait()
        a.beside_own()
        a.give(0, 0)
        g.hand_on(1, 0)
        g.hand_on(1, 1)
        g.get_left(lead)
        g.pair_products(scale)
        g.own_products(scale)
        g.far_left()
        tell(3)
        a.beside_wait(0)
        a.give(0, 1)
        hear(2)
        a.far()
        a.beside_far()
        a.give(1, 0)
        a.hand_on(0, 0)
        a.hand_on(0, 1)
        a.beside_wait(1)
        a.give(1, 1)
        a.hand_on(1, 0)
        a.hand_on(1, 1)
        a.get_left(lead)
        a.pair_products(scale)
        g.spread()
        a.own_products(scale)
    else:
        g.far_left()
        tell(1)
        hear(0)
        g.beside_own()
        for copy in local:
            copy.wait()
        g.beside_far()
        hear(3)
        a.far()
        a.beside_own()
        g.beside_wait(0)
        g.beside_wait(1)
        g.get_left(lead)
        g.pair_products(scale)
        a.far_left()
        tell(2)
        g.own_products(scale)
        a.beside_far()
        a.beside_wait(0)
        a.beside_wait(1)
        a.get_left(lead)
        a.pair_products(scale)
        a.own_products(scale)
        g.spread()
    g.finish()
    a.spread()
    a.finish()
    g.drain()
    a.drain()


def kernel(groups, each, scale, *refs):
    at = Place()
    barrier = pltpu.get_barrier_semaphore()
    peers = [at.flip(name) for name in ("tc", "y", "zh", "tr", "zl")] + [at.flip("tr", "tc")]
    for peer in peers:
        pl.semaphore_signal(barrier, inc=1, device_id=peer, device_id_type=pl.DeviceIdType.MESH)
    pl.semaphore_wait(barrier, len(peers))

    samples, refs = refs[:2], refs[2:]
    olds = (None, None)
    if groups == 1:
        olds, refs = refs[:2], refs[2:]
    totals, scratch, flags = refs[:2], refs[2:-1], refs[-1]
    count = len(scratch) // 2

    def run(lead):
        factors = [
            Factor(at, CHUNKS[i], groups, each[i], samples[i], olds[i], totals[i],
                   scratch[i * count:(i + 1) * count])
            for i in range(2)
        ]
        program(lead, at, *factors, scale, flags)

    lead = at.tr == at.zh
    pl.when(lead)(functools.partial(run, True))
    pl.when(jnp.logical_not(lead))(functools.partial(run, False))


def scratch_of(samples, rows, groups, chunks):
    tokens, width = samples.shape
    lines = 4 * rows
    copies = 3 * chunks + 24
    return [
        pltpu.VMEM((4 * tokens, width), BF16),
        pltpu.VMEM((2, lines, 4 * tokens), BF16),
        pltpu.VMEM((lines, 4 * tokens) if groups > 1 else (16, LANES), BF16),
        pltpu.VMEM((lines, width), BF16),
        pltpu.VMEM((lines, width), BF16),
        pltpu.VMEM((lines, width), F32),
        pltpu.VMEM((lines, width), BF16),
        pltpu.VMEM((lines, width), BF16),
        pltpu.SemaphoreType.DMA((2,)),
        pltpu.SemaphoreType.DMA((copies,)),
        pltpu.SemaphoreType.DMA((copies,)),
        pltpu.SemaphoreType.REGULAR((2,)),
    ]


def body(activations, gradients, old_inputs, old_gradients):
    groups = lax.axis_size("q")
    tokens = activations.shape[0] * lax.axis_size(REPLICA)
    samples, olds = (gradients, activations), (old_gradients, old_inputs)
    each = tuple(old.shape[0] for old in olds)
    scratch = []
    for block, rows, chunks in zip(samples, each, CHUNKS):
        scratch += scratch_of(block, groups * rows, groups, chunks)
    scratch.append(pltpu.SemaphoreType.REGULAR((4,)))
    operands = samples + olds if groups == 1 else samples
    new = pl.pallas_call(
        functools.partial(kernel, groups, each, 1.0 / tokens),
        out_shape=tuple(
            pltpu.VMEM((groups * old.shape[0], old.shape[1]), F32) for old in olds
        ),
        in_specs=[pl.BlockSpec(memory_space=pltpu.HBM)] * len(operands),
        out_specs=(pl.BlockSpec(memory_space=pltpu.VMEM),) * 2,
        scratch_shapes=scratch,
        compiler_params=pltpu.CompilerParams(
            collective_id=0,
            has_side_effects=True,
            vmem_limit_bytes=VMEM if groups == 1 else WIDE_VMEM,
        ),
        name="gram",
    )(*operands)
    if groups > 1:
        new = [lax.psum_scatter(total, "q", scatter_dimension=0, tiled=True) for total in new]
        new = [0.5 * old + 0.5 * total for total, old in zip(new, olds)]
    return new[1], new[0]


def solution(mesh):
    rows = REPLICA + ("tr", "tc")
    return jax.shard_map(
        body,
        mesh=split_mesh(mesh),
        in_specs=(
            P(REPLICA, ("tr", "tc")),
            P(REPLICA, ("tr", "tc")),
            P(rows, None),
            P(rows, None),
        ),
        out_specs=(P(rows, None), P(rows, None)),
        check_vma=False,
    )
```

```python
import functools

import jax
import jax.numpy as jnp
from jax import lax
from jax.experimental import pallas as pl
from jax.experimental.pallas import tpu as pltpu
from jax.sharding import Mesh, PartitionSpec as P

GROUP = (2, 2, 2)
REPLICA = ("q", "zh", "zl", "y")
AXES = REPLICA + ("tr", "tc")
F32, BF16 = jnp.float32, jnp.bfloat16
LANES, STEP = 128, 256
VMEM, WIDE_VMEM = 54 * 2**20, 223 * 2**18
PARTS = 4
PIECES = tuple((t, o, i) for t in range(2) for o in range(2) for i in range(2))
CHUNKS = (4, 2)


def split_mesh(mesh):
    size = mesh.shape["dp"] // 8
    rest = tuple(mesh.shape[name] for name in mesh.axis_names[1:])
    return Mesh(mesh.devices.reshape((size,) + GROUP + rest), AXES)


class Place:
    def __init__(self):
        for name in AXES:
            setattr(self, name, lax.axis_index(name))
        self.replica = self.zh * 4 + self.zl * 2 + self.y
        self.partner = self.zh * 4 + (1 - self.zl) * 2 + self.y

        self.cell = self.tr * 2 + self.tc

    def flip(self, *names):
        return {name: 1 - getattr(self, name) for name in names}


class Factor:
    def __init__(self, at, chunks, groups, each, samples, old, total, refs):
        self.at, self.chunks, self.groups, self.each = at, chunks, groups, each
        self.samples, self.old, self.total = samples, old, total
        (self.wide, self.left, self.left_in, self.pair, self.pair_in, self.sum, self.done,
         self.done_in, self.local_sem, self.send_sem, self.recv_sem, self.ready) = refs
        self.tokens, self.width = samples.shape
        self.lines = self.pair.shape[0]
        self.rows = self.lines // 4
        self.fold = groups == 1
        self.turn = lax.rem(at.tc + at.zl, 2)
        steps = self.width // STEP
        each_part = -(-steps // PARTS)
        self.parts = tuple((low, min(low + each_part, steps)) for low in range(0, steps, each_part))
        keys = [("far", k) for k in range(chunks)]
        keys += [("y", t, k) for t in range(2) for k in range(chunks)]
        keys += [(n,) + piece for n in ("cross", "give", "pass") for piece in PIECES]
        keys += [("pair", p) for p in range(len(self.parts))]
        keys += [("done", p, f) for p in range(len(self.parts)) for f in range(3)]
        keys += [("mix", s, i) for s in range(2) for i in range(2)]
        self.keys = {key: i for i, key in enumerate(keys)}
        self.sent = {}

    def copy(self, key, source, target, device):
        at = self.keys[key]
        return pltpu.make_async_remote_copy(
            src_ref=source,
            dst_ref=target,
            send_sem=self.send_sem.at[at],
            recv_sem=self.recv_sem.at[at],
            device_id=device,
            device_id_type=pl.DeviceIdType.MESH,
        )

    def start(self, key, source, target, device):
        self.sent[key] = self.copy(key, source, target, device)
        self.sent[key].start()

    def leave(self, *key):
        self.sent.pop(key).wait_send()

    def receive(self, key, here):
        self.copy(key, here, here, self.at.flip("tr")).wait_recv()

    def spot(self, t, y, k):
        size = self.tokens // self.chunks
        return self.wide.at[pl.ds(pl.multiple_of((2 * t + y) * self.tokens + k * size, size), size)]

    def own(self, k):
        size = self.tokens // self.chunks
        return self.samples.at[pl.ds(k * size, size)]

    def local(self):
        row = pl.multiple_of(self.at.y * self.tokens, self.tokens)
        target = self.wide.at[pl.ds(row, self.tokens)]
        copies = [pltpu.make_async_copy(self.samples, target, self.local_sem.at[0])]
        if self.fold:
            copies.append(pltpu.make_async_copy(self.old, self.total, self.local_sem.at[1]))
        return copies

    def far(self):
        for k in range(self.chunks):
            self.start(("far", k), self.own(k), self.spot(1, self.at.y, k), self.at.flip("zh"))

    def far_left(self):
        for k in range(self.chunks):
            self.leave("far", k)

    def beside(self, t, k):
        here = self.spot(t, self.at.y, k)
        self.start(("y", t, k), here if t else self.own(k), here, self.at.flip("y"))

    def beside_own(self):
        for k in range(self.chunks):
            self.beside(0, k)

    def beside_left(self):
        for t in range(2):
            for k in range(self.chunks):
                self.leave("y", t, k)

    def beside_far(self, lead):
        each = self.chunks // 2
        for i in range(2):
            for k in range(i * each, (i + 1) * each):
                self.receive(("far", k), self.spot(1, self.at.y, k))
                self.beside(1, k)
            if lead:
                self.give(1, 0, i)

    def beside_wait(self, t):
        for k in range(self.chunks):
            self.receive(("y", t, k), self.spot(t, 1 - self.at.y, k))

    def beside_give(self, t):
        each = self.chunks // 2
        for i in range(2):
            for k in range(i * each, (i + 1) * each):
                self.receive(("y", t, k), self.spot(t, 1 - self.at.y, k))
            self.give(t, 1, i)

    def stretch(self, t, o, i):
        y, size = 1 - self.at.y if o else self.at.y, self.tokens // 2
        return pl.ds(pl.multiple_of((2 * t + y) * self.tokens + i * size, size), size)

    def pick(self, s, replica, tokens):
        at, rows, each = self.at, self.rows, self.each
        span = 4 * each
        window = span if span % LANES == 0 else -(-span // LANES) * LANES + LANES
        line = lax.broadcasted_iota(jnp.int32, (rows, window), 0)
        feature = lax.broadcasted_iota(jnp.int32, (rows, window), 1)
        total = 0.0
        for group in range(self.groups):
            offset = (group * 8 + replica) * span - at.cell * self.width
            start = pl.multiple_of(jnp.clip(offset // LANES * LANES, 0, self.width - window), LANES)
            cells = []
            for cell in range(4):
                hit = feature == line + (offset - start + (cell - group) * each)
                if self.groups > 1:
                    hit &= (line >= group * each) & (line < (group + 1) * each)
                cells.append(jnp.where(hit, 1.0, 0.0).astype(BF16))
            total += lax.dot_general(
                jnp.concatenate(cells, axis=0),
                self.wide[tokens, pl.ds(start, window)],
                (((1,), (1,)), ((), ())),
                preferred_element_type=F32,
            )
        self.left[s, :, tokens] = total.astype(BF16)

    def give(self, t, o, i):
        if self.groups > 1:
            return
        at, tokens = self.at, self.stretch(t, o, i)
        self.pick(self.turn, jnp.where(self.turn == 0, at.replica, at.partner), tokens)
        here = self.left.at[self.turn, :, tokens]
        self.start(("cross", t, o, i), here, here, at.flip("tc"))
        self.start(("give", t, o, i), here, here, at.flip("tr"))

    def give_own(self):
        for i in range(2):
            self.give(0, 0, i)

    def hand_on(self, t, o):
        if self.groups > 1:
            return
        for i in range(2):
            here = self.left.at[1 - self.turn, :, self.stretch(t, o, i)]
            self.receive(("cross", t, o, i), here)
            self.start(("pass", t, o, i), here, here, self.at.flip("tr"))

    def get_left(self, lead):
        at = self.at
        if self.groups == 1:
            if not lead:
                for piece in PIECES:
                    self.receive(("give",) + piece, self.left.at[self.turn, :, self.stretch(*piece)])
                    self.receive(("pass",) + piece, self.left.at[1 - self.turn, :, self.stretch(*piece)])
            return
        for s, replica in ((0, at.replica), (1, at.partner)):
            def block(b, carry, s=s, replica=replica):
                tokens = pl.ds(pl.multiple_of(b * self.tokens, self.tokens), self.tokens)
                self.pick(s, replica, tokens)
                return carry

            lax.fori_loop(0, 4, block, 0)
        for s in range(2):
            for i, name in enumerate(("tr", "tc")):
                other = at.flip(name)
                pl.semaphore_signal(self.ready.at[i], inc=1, device_id=other, device_id_type=pl.DeviceIdType.MESH)
                pl.semaphore_wait(self.ready.at[i], 1)
                self.start(("mix", s, i), self.left.at[s], self.left_in, other)
                self.receive(("mix", s, i), self.left_in)
                self.leave("mix", s, i)

                def add(b, carry, s=s):
                    tokens = pl.ds(pl.multiple_of(b * self.tokens, self.tokens), self.tokens)
                    self.left[s, :, tokens] += self.left_in[:, tokens]
                    return carry

                lax.fori_loop(0, 4, add, 0)

    def columns(self, part):
        low, high = self.parts[part]
        return pl.ds(low * STEP, (high - low) * STEP)

    def steps(self, part, one):
        low, high = self.parts[part]
        lax.fori_loop(low, high, functools.partial(self.step, one), 0)

    def step(self, one, i, carry):
        one(pl.ds(pl.multiple_of(i * STEP, STEP), STEP), i)
        return carry

    def product(self, s, columns):
        return jnp.dot(self.left[s], self.wide[:, columns], preferred_element_type=F32)

    def pair_products(self, scale):
        def one(columns, i):
            self.pair[:, columns] = (self.product(1, columns) * scale).astype(BF16)

        for part in range(len(self.parts)):
            self.steps(part, one)
            here = self.columns(part)
            self.start(("pair", part), self.pair.at[:, here], self.pair_in.at[:, here], self.at.flip("zl"))

    def own_products(self, scale):
        def one(columns, i):
            self.sum[:, columns] = self.product(0, columns) * scale

        lax.fori_loop(0, self.width // STEP, functools.partial(self.step, one), 0)

    def others(self):
        at = self.at
        for f, (up, over) in enumerate(((0, 1), (1, 0), (1, 1))):
            tr = 1 - at.tr if up else at.tr
            tc = 1 - at.tc if over else at.tc
            yield f, {"tr": tr, "tc": tc}, tr * 2 + tc

    def lot(self, cell):
        return pl.ds(pl.multiple_of(cell * self.rows, 16), self.rows)

    def put(self, cell, i, value):
        place = pl.ds(pl.multiple_of(cell * self.width + i * STEP, LANES), STEP)
        self.total[:, place] = 0.5 * self.total[:, place] + 0.5 * value if self.fold else value

    def spread(self):
        at = self.at

        def one(columns, i):
            value = self.sum[:, columns] + self.pair_in[:, columns].astype(F32)
            self.sum[:, columns] = value
            self.done[:, columns] = value.astype(BF16)
            self.put(at.cell, i, self.sum[self.lot(at.cell), columns])

        for part in range(len(self.parts)):
            here = self.columns(part)
            self.receive(("pair", part), self.pair_in.at[:, here])
            self.steps(part, one)
            for f, device, cell in self.others():
                self.start(
                    ("done", part, f),
                    self.done.at[self.lot(cell), here],
                    self.done_in.at[self.lot(at.cell), here],
                    device,
                )

    def finish(self):
        for part in range(len(self.parts)):
            for f, device, cell in self.others():
                def one(columns, i, cell=cell):
                    self.put(cell, i, self.done_in[self.lot(cell), columns].astype(F32))

                self.receive(("done", part, f), self.done_in.at[self.lot(cell), self.columns(part)])
                self.steps(part, one)

    def drain(self):
        for key in list(self.sent):
            self.leave(*key)


def program(lead, at, g, a, scale, flags):
    def tell(i):
        pl.semaphore_signal(flags.at[i], inc=1, device_id=at.flip("tr"), device_id_type=pl.DeviceIdType.MESH)

    def hear(i):
        pl.semaphore_wait(flags.at[i], 1)

    local = g.local() + a.local()
    if not lead:
        g.far()
    for copy in local:
        copy.start()
    if lead:
        g.beside_own()
        local.pop(0).wait()
        g.give_own()
        g.beside_give(0)
        g.beside_far(lead)
        g.beside_give(1)
        g.beside_left()
        tell(0)
        hear(1)
        g.far()
        g.hand_on(0, 0)
        g.hand_on(0, 1)
        for copy in local:
            copy.wait()
        a.beside_own()
        a.give_own()
        g.hand_on(1, 0)
        g.hand_on(1, 1)
        g.get_left(lead)
        g.pair_products(scale)
        g.own_products(scale)
        g.far_left()
        tell(3)
        a.beside_give(0)
        hear(2)
        a.far()
        a.beside_far(lead)
        a.hand_on(0, 0)
        a.hand_on(0, 1)
        a.beside_give(1)
        a.hand_on(1, 0)
        a.hand_on(1, 1)
        a.get_left(lead)
        a.pair_products(scale)
        g.spread()
        a.own_products(scale)
    else:
        g.far_left()
        tell(1)
        hear(0)
        g.beside_own()
        for copy in local:
            copy.wait()
        g.beside_far(lead)
        hear(3)
        a.far()
        a.beside_own()
        g.beside_wait(0)
        g.beside_wait(1)
        g.get_left(lead)
        g.pair_products(scale)
        a.far_left()
        tell(2)
        g.own_products(scale)
        a.beside_far(lead)
        a.beside_wait(0)
        a.beside_wait(1)
        a.get_left(lead)
        a.pair_products(scale)
        a.own_products(scale)
        g.spread()
    g.finish()
    a.spread()
    a.finish()
    g.drain()
    a.drain()


def kernel(groups, each, scale, *refs):
    at = Place()
    barrier = pltpu.get_barrier_semaphore()
    peers = [at.flip(name) for name in ("tc", "y", "zh", "tr", "zl")] + [at.flip("tr", "tc")]
    for peer in peers:
        pl.semaphore_signal(barrier, inc=1, device_id=peer, device_id_type=pl.DeviceIdType.MESH)
    pl.semaphore_wait(barrier, len(peers))

    samples, refs = refs[:2], refs[2:]
    olds = (None, None)
    if groups == 1:
        olds, refs = refs[:2], refs[2:]
    totals, scratch, flags = refs[:2], refs[2:-1], refs[-1]
    count = len(scratch) // 2

    def run(lead):
        factors = [
            Factor(at, CHUNKS[i], groups, each[i], samples[i], olds[i], totals[i],
                   scratch[i * count:(i + 1) * count])
            for i in range(2)
        ]
        program(lead, at, *factors, scale, flags)

    lead = at.tr == at.zh
    pl.when(lead)(functools.partial(run, True))
    pl.when(jnp.logical_not(lead))(functools.partial(run, False))


def scratch_of(samples, rows, groups, chunks):
    tokens, width = samples.shape
    lines = 4 * rows
    copies = 3 * chunks + len(PIECES) * 3 + 4 * PARTS + 4
    return [
        pltpu.VMEM((4 * tokens, width), BF16),
        pltpu.VMEM((2, lines, 4 * tokens), BF16),
        pltpu.VMEM((lines, 4 * tokens) if groups > 1 else (16, LANES), BF16),
        pltpu.VMEM((lines, width), BF16),
        pltpu.VMEM((lines, width), BF16),
        pltpu.VMEM((lines, width), F32),
        pltpu.VMEM((lines, width), BF16),
        pltpu.VMEM((lines, width), BF16),
        pltpu.SemaphoreType.DMA((2,)),
        pltpu.SemaphoreType.DMA((copies,)),
        pltpu.SemaphoreType.DMA((copies,)),
        pltpu.SemaphoreType.REGULAR((2,)),
    ]


def body(activations, gradients, old_inputs, old_gradients):
    groups = lax.axis_size("q")
    tokens = activations.shape[0] * lax.axis_size(REPLICA)
    samples, olds = (gradients, activations), (old_gradients, old_inputs)
    each = tuple(old.shape[0] for old in olds)
    scratch = []
    for block, rows, chunks in zip(samples, each, CHUNKS):
        scratch += scratch_of(block, groups * rows, groups, chunks)
    scratch.append(pltpu.SemaphoreType.REGULAR((4,)))
    operands = samples + olds if groups == 1 else samples
    new = pl.pallas_call(
        functools.partial(kernel, groups, each, 1.0 / tokens),
        out_shape=tuple(
            pltpu.VMEM((groups * old.shape[0], old.shape[1]), F32) for old in olds
        ),
        in_specs=[pl.BlockSpec(memory_space=pltpu.HBM)] * len(operands),
        out_specs=(pl.BlockSpec(memory_space=pltpu.VMEM),) * 2,
        scratch_shapes=scratch,
        compiler_params=pltpu.CompilerParams(
            collective_id=0,
            has_side_effects=True,
            vmem_limit_bytes=VMEM if groups == 1 else WIDE_VMEM,
        ),
        name="gram",
    )(*operands)
    if groups > 1:
        new = [lax.psum_scatter(total, "q", scatter_dimension=0, tiled=True) for total in new]
        new = [0.5 * old + 0.5 * total for total, old in zip(new, olds)]
    return new[1], new[0]


def solution(mesh):
    rows = REPLICA + ("tr", "tc")
    return jax.shard_map(
        body,
        mesh=split_mesh(mesh),
        in_specs=(
            P(REPLICA, ("tr", "tc")),
            P(REPLICA, ("tr", "tc")),
            P(rows, None),
            P(rows, None),
        ),
        out_specs=(P(rows, None), P(rows, None)),
        check_vma=False,
    )
```

```python
import functools

import jax
import jax.numpy as jnp
from jax import lax
from jax.experimental import pallas as pl
from jax.experimental.pallas import tpu as pltpu
from jax.sharding import Mesh, PartitionSpec as P

GROUP = (2, 2, 2)
REPLICA = ("q", "zh", "zl", "y")
AXES = REPLICA + ("tr", "tc")
F32, BF16 = jnp.float32, jnp.bfloat16
LANES, STEP = 128, 256
VMEM, WIDE_VMEM = 54 * 2**20, 223 * 2**18
PARTS = 4
PIECES = tuple((t, o, i) for t in range(2) for o in range(2) for i in range(2))
CHUNKS = (4, 2)


def split_mesh(mesh):
    size = mesh.shape["dp"] // 8
    rest = tuple(mesh.shape[name] for name in mesh.axis_names[1:])
    return Mesh(mesh.devices.reshape((size,) + GROUP + rest), AXES)


class Place:
    def __init__(self):
        for name in AXES:
            setattr(self, name, lax.axis_index(name))
        self.replica = self.zh * 4 + self.zl * 2 + self.y
        self.partner = self.zh * 4 + (1 - self.zl) * 2 + self.y

        self.cell = self.tr * 2 + self.tc

    def flip(self, *names):
        return {name: 1 - getattr(self, name) for name in names}


class Factor:
    def __init__(self, at, chunks, groups, each, samples, old, total, refs):
        self.at, self.chunks, self.groups, self.each = at, chunks, groups, each
        self.samples, self.old, self.total = samples, old, total
        (self.wide, self.left, self.left_in, self.pair, self.pair_in, self.sum, self.done,
         self.done_in, self.local_sem, self.send_sem, self.recv_sem, self.ready) = refs
        self.tokens, self.width = samples.shape
        self.lines = self.pair.shape[0]
        self.rows = self.lines // 4
        self.fold = groups == 1
        self.turn = lax.rem(at.tc + at.zl, 2)
        steps = self.width // STEP
        each_part = -(-steps // PARTS)
        first = steps - (steps - 1) // each_part * each_part
        ends = tuple(range(first, steps + 1, each_part))
        self.parts = tuple(zip((0,) + ends, ends))
        keys = [("far", k) for k in range(chunks)]
        keys += [("y", t, k) for t in range(2) for k in range(chunks)]
        keys += [(n,) + piece for n in ("cross", "give", "pass") for piece in PIECES]
        keys += [("pair", p) for p in range(len(self.parts))]
        keys += [("done", p, f) for p in range(len(self.parts)) for f in range(3)]
        keys += [("mix", s, i) for s in range(2) for i in range(2)]
        self.keys = {key: i for i, key in enumerate(keys)}
        self.sent = {}

    def copy(self, key, source, target, device):
        at = self.keys[key]
        return pltpu.make_async_remote_copy(
            src_ref=source,
            dst_ref=target,
            send_sem=self.send_sem.at[at],
            recv_sem=self.recv_sem.at[at],
            device_id=device,
            device_id_type=pl.DeviceIdType.MESH,
        )

    def start(self, key, source, target, device):
        self.sent[key] = self.copy(key, source, target, device)
        self.sent[key].start()

    def leave(self, *key):
        self.sent.pop(key).wait_send()

    def receive(self, key, here):
        self.copy(key, here, here, self.at.flip("tr")).wait_recv()

    def spot(self, t, y, k):
        size = self.tokens // self.chunks
        return self.wide.at[pl.ds(pl.multiple_of((2 * t + y) * self.tokens + k * size, size), size)]

    def own(self, k):
        size = self.tokens // self.chunks
        return self.samples.at[pl.ds(k * size, size)]

    def local(self):
        row = pl.multiple_of(self.at.y * self.tokens, self.tokens)
        target = self.wide.at[pl.ds(row, self.tokens)]
        copies = [pltpu.make_async_copy(self.samples, target, self.local_sem.at[0])]
        if self.fold:
            copies.append(pltpu.make_async_copy(self.old, self.total, self.local_sem.at[1]))
        return copies

    def far(self):
        for k in range(self.chunks):
            self.start(("far", k), self.own(k), self.spot(1, self.at.y, k), self.at.flip("zh"))

    def far_left(self):
        for k in range(self.chunks):
            self.leave("far", k)

    def beside(self, t, k):
        here = self.spot(t, self.at.y, k)
        self.start(("y", t, k), here if t else self.own(k), here, self.at.flip("y"))

    def beside_own(self):
        for k in range(self.chunks):
            self.beside(0, k)

    def beside_left(self):
        for t in range(2):
            for k in range(self.chunks):
                self.leave("y", t, k)

    def beside_far(self, lead):
        each = self.chunks // 2
        for i in range(2):
            for k in range(i * each, (i + 1) * each):
                self.receive(("far", k), self.spot(1, self.at.y, k))
                self.beside(1, k)
            if lead:
                self.give(1, 0, i)

    def beside_wait(self, t):
        for k in range(self.chunks):
            self.receive(("y", t, k), self.spot(t, 1 - self.at.y, k))

    def beside_give(self, t):
        each = self.chunks // 2
        for i in range(2):
            for k in range(i * each, (i + 1) * each):
                self.receive(("y", t, k), self.spot(t, 1 - self.at.y, k))
            self.give(t, 1, i)

    def stretch(self, t, o, i):
        y, size = 1 - self.at.y if o else self.at.y, self.tokens // 2
        return pl.ds(pl.multiple_of((2 * t + y) * self.tokens + i * size, size), size)

    def pick(self, s, replica, tokens):
        at, rows, each = self.at, self.rows, self.each
        span = 4 * each
        window = span if span % LANES == 0 else -(-span // LANES) * LANES + LANES
        line = lax.broadcasted_iota(jnp.int32, (rows, window), 0)
        feature = lax.broadcasted_iota(jnp.int32, (rows, window), 1)
        total = 0.0
        for group in range(self.groups):
            offset = (group * 8 + replica) * span - at.cell * self.width
            start = pl.multiple_of(jnp.clip(offset // LANES * LANES, 0, self.width - window), LANES)
            cells = []
            for cell in range(4):
                hit = feature == line + (offset - start + (cell - group) * each)
                if self.groups > 1:
                    hit &= (line >= group * each) & (line < (group + 1) * each)
                cells.append(jnp.where(hit, 1.0, 0.0).astype(BF16))
            total += lax.dot_general(
                jnp.concatenate(cells, axis=0),
                self.wide[tokens, pl.ds(start, window)],
                (((1,), (1,)), ((), ())),
                preferred_element_type=F32,
            )
        self.left[s, :, tokens] = total.astype(BF16)

    def give(self, t, o, i):
        if self.groups > 1:
            return
        at, tokens = self.at, self.stretch(t, o, i)
        self.pick(self.turn, jnp.where(self.turn == 0, at.replica, at.partner), tokens)
        here = self.left.at[self.turn, :, tokens]
        self.start(("cross", t, o, i), here, here, at.flip("tc"))
        self.start(("give", t, o, i), here, here, at.flip("tr"))

    def give_own(self):
        for i in range(2):
            self.give(0, 0, i)

    def hand_on(self, t, o):
        if self.groups > 1:
            return
        for i in range(2):
            here = self.left.at[1 - self.turn, :, self.stretch(t, o, i)]
            self.receive(("cross", t, o, i), here)
            self.start(("pass", t, o, i), here, here, self.at.flip("tr"))

    def get_left(self, lead):
        at = self.at
        if self.groups == 1:
            if not lead:
                for piece in PIECES:
                    self.receive(("give",) + piece, self.left.at[self.turn, :, self.stretch(*piece)])
                    self.receive(("pass",) + piece, self.left.at[1 - self.turn, :, self.stretch(*piece)])
            return
        for s, replica in ((0, at.replica), (1, at.partner)):
            def block(b, carry, s=s, replica=replica):
                tokens = pl.ds(pl.multiple_of(b * self.tokens, self.tokens), self.tokens)
                self.pick(s, replica, tokens)
                return carry

            lax.fori_loop(0, 4, block, 0)
        for s in range(2):
            for i, name in enumerate(("tr", "tc")):
                other = at.flip(name)
                pl.semaphore_signal(self.ready.at[i], inc=1, device_id=other, device_id_type=pl.DeviceIdType.MESH)
                pl.semaphore_wait(self.ready.at[i], 1)
                self.start(("mix", s, i), self.left.at[s], self.left_in, other)
                self.receive(("mix", s, i), self.left_in)
                self.leave("mix", s, i)

                def add(b, carry, s=s):
                    tokens = pl.ds(pl.multiple_of(b * self.tokens, self.tokens), self.tokens)
                    self.left[s, :, tokens] += self.left_in[:, tokens]
                    return carry

                lax.fori_loop(0, 4, add, 0)

    def columns(self, part):
        low, high = self.parts[part]
        return pl.ds(low * STEP, (high - low) * STEP)

    def steps(self, part, one):
        low, high = self.parts[part]
        lax.fori_loop(low, high, functools.partial(self.step, one), 0)

    def step(self, one, i, carry):
        one(pl.ds(pl.multiple_of(i * STEP, STEP), STEP), i)
        return carry

    def product(self, s, columns):
        return jnp.dot(self.left[s], self.wide[:, columns], preferred_element_type=F32)

    def pair_products(self, scale):
        def one(columns, i):
            self.pair[:, columns] = (self.product(1, columns) * scale).astype(BF16)

        for part in range(len(self.parts)):
            self.steps(part, one)
            here = self.columns(part)
            self.start(("pair", part), self.pair.at[:, here], self.pair_in.at[:, here], self.at.flip("zl"))

    def own_products(self, scale):
        def one(columns, i):
            self.sum[:, columns] = self.product(0, columns) * scale

        lax.fori_loop(0, self.width // STEP, functools.partial(self.step, one), 0)

    def others(self):
        at = self.at
        for f, (up, over) in enumerate(((0, 1), (1, 0), (1, 1))):
            tr = 1 - at.tr if up else at.tr
            tc = 1 - at.tc if over else at.tc
            yield f, {"tr": tr, "tc": tc}, tr * 2 + tc

    def lot(self, cell):
        return pl.ds(pl.multiple_of(cell * self.rows, 16), self.rows)

    def put(self, cell, i, value):
        place = pl.ds(pl.multiple_of(cell * self.width + i * STEP, LANES), STEP)
        self.total[:, place] = 0.5 * self.total[:, place] + 0.5 * value if self.fold else value

    def spread(self):
        at = self.at

        def one(columns, i):
            value = self.sum[:, columns] + self.pair_in[:, columns].astype(F32)
            self.sum[:, columns] = value
            self.done[:, columns] = value.astype(BF16)
            self.put(at.cell, i, self.sum[self.lot(at.cell), columns])

        for part in range(len(self.parts)):
            here = self.columns(part)
            self.receive(("pair", part), self.pair_in.at[:, here])
            self.steps(part, one)
            for f, device, cell in self.others():
                self.start(
                    ("done", part, f),
                    self.done.at[self.lot(cell), here],
                    self.done_in.at[self.lot(at.cell), here],
                    device,
                )

    def finish(self):
        for part in range(len(self.parts)):
            for f, device, cell in self.others():
                def one(columns, i, cell=cell):
                    self.put(cell, i, self.done_in[self.lot(cell), columns].astype(F32))

                self.receive(("done", part, f), self.done_in.at[self.lot(cell), self.columns(part)])
                self.steps(part, one)

    def drain(self):
        for key in list(self.sent):
            self.leave(*key)


def program(lead, at, g, a, scale, flags):
    def tell(i):
        pl.semaphore_signal(flags.at[i], inc=1, device_id=at.flip("tr"), device_id_type=pl.DeviceIdType.MESH)

    def hear(i):
        pl.semaphore_wait(flags.at[i], 1)

    local = g.local() + a.local()
    if not lead:
        g.far()
    if lead:
        g.beside_own()
    for copy in local:
        copy.start()
    if lead:
        local.pop(0).wait()
        g.give_own()
        g.beside_give(0)
        g.beside_far(lead)
        g.beside_give(1)
        g.beside_left()
        tell(0)
        hear(1)
        g.far()
        g.hand_on(0, 0)
        g.hand_on(0, 1)
        for copy in local:
            copy.wait()
        a.beside_own()
        a.give_own()
        g.hand_on(1, 0)
        g.hand_on(1, 1)
        g.get_left(lead)
        g.pair_products(scale)
        g.own_products(scale)
        g.far_left()
        tell(3)
        a.beside_give(0)
        hear(2)
        a.far()
        a.beside_far(lead)
        a.hand_on(0, 0)
        a.hand_on(0, 1)
        a.beside_give(1)
        a.hand_on(1, 0)
        a.hand_on(1, 1)
        a.get_left(lead)
        a.pair_products(scale)
        g.spread()
        a.own_products(scale)
    else:
        g.far_left()
        tell(1)
        hear(0)
        g.beside_own()
        for copy in local:
            copy.wait()
        g.beside_far(lead)
        hear(3)
        a.far()
        a.beside_own()
        g.beside_wait(0)
        g.beside_wait(1)
        g.get_left(lead)
        g.pair_products(scale)
        a.far_left()
        tell(2)
        g.own_products(scale)
        a.beside_far(lead)
        a.beside_wait(0)
        a.beside_wait(1)
        a.get_left(lead)
        a.pair_products(scale)
        a.own_products(scale)
        g.spread()
    g.finish()
    a.spread()
    a.finish()
    g.drain()
    a.drain()


def kernel(groups, each, scale, *refs):
    at = Place()
    barrier = pltpu.get_barrier_semaphore()
    peers = [at.flip(name) for name in ("tc", "y", "zh", "tr", "zl")] + [at.flip("tr", "tc")]
    for peer in peers:
        pl.semaphore_signal(barrier, inc=1, device_id=peer, device_id_type=pl.DeviceIdType.MESH)
    pl.semaphore_wait(barrier, len(peers))

    samples, refs = refs[:2], refs[2:]
    olds = (None, None)
    if groups == 1:
        olds, refs = refs[:2], refs[2:]
    totals, scratch, flags = refs[:2], refs[2:-1], refs[-1]
    count = len(scratch) // 2

    def run(lead):
        factors = [
            Factor(at, CHUNKS[i], groups, each[i], samples[i], olds[i], totals[i],
                   scratch[i * count:(i + 1) * count])
            for i in range(2)
        ]
        program(lead, at, *factors, scale, flags)

    lead = at.tr == at.zh
    pl.when(lead)(functools.partial(run, True))
    pl.when(jnp.logical_not(lead))(functools.partial(run, False))


def scratch_of(samples, rows, groups, chunks):
    tokens, width = samples.shape
    lines = 4 * rows
    copies = 3 * chunks + len(PIECES) * 3 + 4 * PARTS + 4
    return [
        pltpu.VMEM((4 * tokens, width), BF16),
        pltpu.VMEM((2, lines, 4 * tokens), BF16),
        pltpu.VMEM((lines, 4 * tokens) if groups > 1 else (16, LANES), BF16),
        pltpu.VMEM((lines, width), BF16),
        pltpu.VMEM((lines, width), BF16),
        pltpu.VMEM((lines, width), F32),
        pltpu.VMEM((lines, width), BF16),
        pltpu.VMEM((lines, width), BF16),
        pltpu.SemaphoreType.DMA((2,)),
        pltpu.SemaphoreType.DMA((copies,)),
        pltpu.SemaphoreType.DMA((copies,)),
        pltpu.SemaphoreType.REGULAR((2,)),
    ]


def body(activations, gradients, old_inputs, old_gradients):
    groups = lax.axis_size("q")
    tokens = activations.shape[0] * lax.axis_size(REPLICA)
    samples, olds = (gradients, activations), (old_gradients, old_inputs)
    each = tuple(old.shape[0] for old in olds)
    scratch = []
    for block, rows, chunks in zip(samples, each, CHUNKS):
        scratch += scratch_of(block, groups * rows, groups, chunks)
    scratch.append(pltpu.SemaphoreType.REGULAR((4,)))
    operands = samples + olds if groups == 1 else samples
    new = pl.pallas_call(
        functools.partial(kernel, groups, each, 1.0 / tokens),
        out_shape=tuple(
            pltpu.VMEM((groups * old.shape[0], old.shape[1]), F32) for old in olds
        ),
        in_specs=[pl.BlockSpec(memory_space=pltpu.HBM)] * len(operands),
        out_specs=(pl.BlockSpec(memory_space=pltpu.VMEM),) * 2,
        scratch_shapes=scratch,
        compiler_params=pltpu.CompilerParams(
            collective_id=0,
            has_side_effects=True,
            vmem_limit_bytes=VMEM if groups == 1 else WIDE_VMEM,
        ),
        name="gram",
    )(*operands)
    if groups > 1:
        new = [lax.psum_scatter(total, "q", scatter_dimension=0, tiled=True) for total in new]
        new = [0.5 * old + 0.5 * total for total, old in zip(new, olds)]
    return new[1], new[0]


def solution(mesh):
    rows = REPLICA + ("tr", "tc")
    return jax.shard_map(
        body,
        mesh=split_mesh(mesh),
        in_specs=(
            P(REPLICA, ("tr", "tc")),
            P(REPLICA, ("tr", "tc")),
            P(rows, None),
            P(rows, None),
        ),
        out_specs=(P(rows, None), P(rows, None)),
        check_vma=False,
    )
```
